256 devices in a mesh: dp: 128 (over x, z, y_hi, core), outer: 2 (over y_lo).
Axes of the slice: x: 4, y: 4 (y_hi: 2, y_lo: 2; y = y_hi * 2 + y_lo), z: 8, core: 2. Of those that a mesh axis runs over, the one named last changes fastest.
Arguments:
- images: bfloat16 [16384, 1024], P('dp'), may hold values from -8 to 8
- texts: bfloat16 [16384, 1024], P(('dp', 'outer')), may hold values from -8 to 8
- logit_scale: float32 [1], replicated, may hold values from 70 to 100
Outputs:
- image_loss: float32 [16384], P(('dp', 'outer'))
- text_loss: float32 [16384], P(('dp', 'outer'))
The draws below stay inside these ranges and needn't reach their ends.
All inputs are finite; a program needn't handle non-finite values.
Results may differ from the reference program's by a relative error of at most 0.003.
Values may be sent and summed in bfloat16 or wider, within the bound.
No kernel may reach another device: no remote copies, remote signals or barrier semaphores. Data moves between devices by JAX's collectives and lax.ppermute only.
A program may use at most 64 MiB of HBM per device.

```python
import math
import jax
import jax.numpy as jnp
from jax import lax

D = 1024
BATCH = 16384


def raw_features(key, salt):
    normal_draw = jax.random.normal(jax.random.fold_in(key, salt), (BATCH, D), jnp.float32)
    return jnp.clip(normal_draw, -8.0, 8.0)


def draw_images(key, part):
    return raw_features(key, 1).astype(jnp.bfloat16)


def draw_texts(key, part):
    own_texts = raw_features(key, 2)
    return own_texts.astype(jnp.bfloat16)


def draw_logit_scale(key, part):
    return jax.random.uniform(jax.random.fold_in(key, 3), (1,), jnp.float32, 70.0, 100.0)


def setup_inputs(seed: int = 0) -> dict:
    streams_of = jax.random.split(jax.random.key(seed), 4)
    images = draw_images(jax.random.fold_in(streams_of[3], 71), 0)
    texts = draw_texts(jax.random.fold_in(streams_of[3], 71), 0)
    logit_scale = draw_logit_scale(jax.random.fold_in(streams_of[3], 71), 0)
    return dict(images=images, texts=texts, logit_scale=logit_scale)


def normalise(features):
    widened = features.astype(jnp.float32)
    return (widened * lax.rsqrt(lax.optimization_barrier(jnp.sum(widened * widened, axis=1, keepdims=True)) + 1.0)).astype(jnp.bfloat16)

def reference(images, texts, logit_scale):
    image_unit = normalise(images)
    text_unit = normalise(texts)
    factor = logit_scale[0]
    block_size = math.gcd(BATCH, 1024)
    text_blocks = text_unit.reshape(BATCH // block_size, block_size, D)

    def absorb_block(states, text_block):
        row_peak, row_total = states
        scores = jnp.einsum('id,jd->ij', image_unit, text_block, preferred_element_type=jnp.float32) * factor
        col_peak = lax.optimization_barrier(jnp.max(scores, axis=0))
        col_lse = col_peak + jnp.log(lax.optimization_barrier(jnp.sum(jnp.exp(scores - col_peak), axis=0)))
        new_peak = jnp.maximum(row_peak, lax.optimization_barrier(jnp.max(scores, axis=1)))
        row_total = row_total * jnp.exp(row_peak - new_peak) + lax.optimization_barrier(jnp.sum(jnp.exp(scores - new_peak[:, None]), axis=1))
        return ((new_peak, row_total), col_lse)
    initial = (jnp.full((BATCH,), -1e+30, jnp.float32), jnp.zeros((BATCH,), jnp.float32))
    (row_peak, row_total), col_lse = lax.scan(absorb_block, initial, text_blocks)
    diagonal = lax.optimization_barrier(jnp.sum(image_unit.astype(jnp.float32) * text_unit.astype(jnp.float32), axis=1)) * factor
    image_loss = row_peak + jnp.log(row_total) - diagonal
    text_loss = col_lse.reshape(BATCH) - diagonal
    return (image_loss, text_loss)
```

```python
import math

import jax
import jax.numpy as jnp
from jax import lax
from jax.experimental import pallas as pl
from jax.experimental.pallas import tpu as pltpu
from jax.sharding import Mesh
from jax.sharding import PartitionSpec as P


HIGH = 40.0
LOW = -60.0
LOG2E = math.log2(math.e)
VMEM = pl.BlockSpec(memory_space=pltpu.VMEM)
SMEM = pl.BlockSpec(memory_space=pltpu.SMEM)
FLIP_Y = ((0, 3), (3, 0), (1, 2), (2, 1))


def normalise_kernel(images_ref, texts_ref, image_unit_ref, text_unit_ref):
    for source, target in ((images_ref, image_unit_ref), (texts_ref, text_unit_ref)):
        wide = source[...].astype(jnp.float32)
        squares = jnp.sum(wide * wide, axis=1, keepdims=True)
        target[...] = (wide * lax.rsqrt(squares + 1.0)).astype(jnp.bfloat16)


def normalise(images, texts):
    return pl.pallas_call(
        normalise_kernel,
        out_shape=(
            jax.ShapeDtypeStruct(images.shape, jnp.bfloat16),
            jax.ShapeDtypeStruct(texts.shape, jnp.bfloat16),
        ),
        in_specs=[VMEM, VMEM],
        out_specs=(VMEM, VMEM),
        compiler_params=pltpu.CompilerParams(vmem_limit_bytes=8 << 20),
    )(images, texts)


def block_kernel(scale_ref, image_ref, text_ref, row_ref, col_ref, row_high, row_low, col_high, col_low):
    tile = 256
    half_scale = scale_ref[0] * (0.5 * LOG2E)
    cut = math.exp(-HIGH / 2)
    lift = math.exp((HIGH - LOW) / 2)
    rows, cols = image_ref.shape[0], text_ref.shape[0]
    for r in range(rows // tile):
        high_sum = low_sum = None
        for c in range(cols // tile):
            dots = lax.dot_general(
                image_ref[r * tile : (r + 1) * tile, :],
                text_ref[c * tile : (c + 1) * tile, :],
                (((1,), (1,)), ((), ())),
                preferred_element_type=jnp.float32,
            )
            root = jnp.exp2(dots * half_scale - (HIGH / 2 * LOG2E))
            high = root * root
            low = jnp.minimum(root, cut) * lift
            low = low * low
            high_part = high[:, :128] + high[:, 128:]
            low_part = low[:, :128] + low[:, 128:]
            high_sum = high_part if high_sum is None else high_sum + high_part
            low_sum = low_part if low_sum is None else low_sum + low_part
            at = slice(c * tile, (c + 1) * tile)
            high_col = jnp.sum(high.reshape(tile // 8, 8, tile), axis=0)
            low_col = jnp.sum(low.reshape(tile // 8, 8, tile), axis=0)
            if r == 0:
                col_high[:, at] = high_col
                col_low[:, at] = low_col
            else:
                col_high[:, at] += high_col
                col_low[:, at] += low_col
        for i in range(tile // 128):
            piece = r * (tile // 128) + i
            part = slice(i * 128, (i + 1) * 128)
            row_ref[2 * piece : 2 * piece + 1, :] = jnp.sum(high_sum[part].T, axis=0, keepdims=True)
            row_ref[2 * piece + 1 : 2 * piece + 2, :] = jnp.sum(low_sum[part].T, axis=0, keepdims=True)
    half = cols // 2
    for e in range(2):
        at = slice(e * half, (e + 1) * half)
        col_ref[2 * e : 2 * e + 1, :] = jnp.sum(col_high[:, at], axis=0, keepdims=True)
        col_ref[2 * e + 1 : 2 * e + 2, :] = jnp.sum(col_low[:, at], axis=0, keepdims=True)


def block_sums(logit_scale, images, texts):
    rows, cols, depth = images.shape[0], texts.shape[0], images.shape[1]
    return pl.pallas_call(
        block_kernel,
        out_shape=(
            jax.ShapeDtypeStruct((rows // 64, 128), jnp.float32),
            jax.ShapeDtypeStruct((4, cols // 2), jnp.float32),
        ),
        in_specs=[SMEM, VMEM, VMEM],
        out_specs=(VMEM, VMEM),
        scratch_shapes=[
            pltpu.VMEM((rows, 128), jnp.float32),
            pltpu.VMEM((rows, 128), jnp.float32),
            pltpu.VMEM((8, cols), jnp.float32),
            pltpu.VMEM((8, cols), jnp.float32),
        ],
        compiler_params=pltpu.CompilerParams(vmem_limit_bytes=24 << 20),
        cost_estimate=pl.CostEstimate(
            flops=2 * rows * cols * depth,
            bytes_accessed=2 * (rows + cols) * depth,
            transcendentals=rows * cols,
        ),
    )(logit_scale, images, texts)


def fetch(block, axis, size, apart):
    return lax.ppermute(block, axis, [((i + apart) % size, i) for i in range(size)])


def send(block, axis, size, apart):
    return fetch(block, axis, size, -apart)


def gather_images(own):
    flip = lax.ppermute(own, ("yh", "yl"), FLIP_Y)
    half = own.shape[0] // 2
    above = fetch(own, "x", 4, 1)
    below = fetch(own, "x", 4, -1)
    far_above = fetch(jnp.concatenate([flip, above[:half]], 0), "x", 4, 1)
    far_below = fetch(jnp.concatenate([flip, below[half:]], 0), "x", 4, -1)
    rows = 2 * half
    flip_above, flip_below = far_above[:rows], far_below[:rows]
    flip_far_a = fetch(flip_above[:half], "x", 4, 1)
    flip_far_b = fetch(flip_below[half:], "x", 4, -1)
    return jnp.concatenate(
        [own, flip, above, flip_above, far_above[rows:], far_below[rows:], flip_far_a, flip_far_b, below, flip_below],
        0,
    )


def gather_texts(own):
    half = own.shape[0] // 2
    p2, m2 = fetch(own, "z", 8, 2), fetch(own, "z", 8, -2)
    p1, m1 = fetch(own, "z", 8, 1), fetch(own, "z", 8, -1)
    p3, m3 = fetch(p2, "z", 8, 1), fetch(m2, "z", 8, -1)
    p4, m4 = fetch(p2[:half], "z", 8, 2), fetch(m2[half:], "z", 8, -2)
    mine = jnp.concatenate([own, p1, p2, p3, p4, m4, m3, m2, m1], 0)
    other = lax.ppermute(mine, "c", ((0, 1), (1, 0)))
    return jnp.concatenate([mine, other], 0)


def reduce_rows(sums):
    total = sums[:4]
    for apart in (1, 3, 2):
        total = total + send(sums[4 * apart : 4 * apart + 4], "x", 4, apart)
    total = total[:2] + lax.ppermute(total[2:], ("yh", "yl"), FLIP_Y)
    yl = lax.axis_index("yl")
    low, high = total[:, :64], total[:, 64:]
    keep = jnp.where(yl == 0, low, high)
    away = jnp.where(yl == 0, high, low)
    return keep + lax.ppermute(away, "yl", ((0, 1), (1, 0)))


def reduce_cols(sums):
    total = sums[:2] + lax.ppermute(sums[2:], "c", ((0, 1), (1, 0)))
    part = [total[:, 64 * i : 64 * i + 64] for i in range(8)]
    up = send(jnp.concatenate([part[1], part[3]], 0), "z", 8, 1)
    down = send(jnp.concatenate([part[7], part[5]], 0), "z", 8, -1)
    here = part[0] + up[:2] + down[:2]
    two = part[2] + up[2:]
    minus_two = part[6] + down[2:]
    return here + send(two, "z", 8, 2) + send(minus_two, "z", 8, -2) + send(part[4], "z", 8, 4)


def log_sum(sums):
    high, low = sums[0], sums[1]
    return jnp.where(high > math.exp(-HIGH), jnp.log(high) + HIGH, jnp.log(low) + LOW)


def on_device(images, texts, logit_scale):
    image_unit, text_unit = normalise(images, texts)
    rows = text_unit.shape[0]
    all_images = gather_images(image_unit)
    all_texts = gather_texts(text_unit)
    row_sums, col_sums = block_sums(logit_scale, all_images, all_texts)
    image_own = lax.dynamic_slice_in_dim(image_unit, lax.axis_index("yl") * rows, rows, 0)
    diagonal = (
        jnp.sum(image_own.astype(jnp.float32) * text_unit.astype(jnp.float32), axis=1) * logit_scale[0]
    )
    image_lse = log_sum(reduce_rows(row_sums))
    text_lse = log_sum(reduce_cols(col_sums))
    return (image_lse - diagonal, text_lse - diagonal)


def solution(mesh):
    fine = Mesh(mesh.devices.reshape(4, 8, 2, 2, 2), ("x", "z", "yh", "c", "yl"))
    dp = ("x", "z", "yh", "c")
    in_specs = (P(dp, None), P(dp + ("yl",), None), P())
    out_specs = (P(dp + ("yl",)), P(dp + ("yl",)))
    return jax.shard_map(
        on_device, mesh=fine, in_specs=in_specs, out_specs=out_specs, check_vma=False
    )
```

```python
import math

import jax
import jax.numpy as jnp
from jax import lax
from jax.experimental import pallas as pl
from jax.experimental.pallas import tpu as pltpu
from jax.sharding import Mesh
from jax.sharding import PartitionSpec as P


HIGH = 40.0
LOW = -60.0
LOG2E = math.log2(math.e)
VMEM = pl.BlockSpec(memory_space=pltpu.VMEM)
SMEM = pl.BlockSpec(memory_space=pltpu.SMEM)
FLIP_Y = ((0, 3), (3, 0), (1, 2), (2, 1))


def normalise_kernel(images_ref, texts_ref, image_unit_ref, text_unit_ref):
    for source, target in ((images_ref, image_unit_ref), (texts_ref, text_unit_ref)):
        wide = source[...].astype(jnp.float32)
        squares = jnp.sum(wide * wide, axis=1, keepdims=True)
        target[...] = (wide * lax.rsqrt(squares + 1.0)).astype(jnp.bfloat16)


def normalise(images, texts):
    return pl.pallas_call(
        normalise_kernel,
        out_shape=(
            jax.ShapeDtypeStruct(images.shape, jnp.bfloat16),
            jax.ShapeDtypeStruct(texts.shape, jnp.bfloat16),
        ),
        in_specs=[VMEM, VMEM],
        out_specs=(VMEM, VMEM),
        compiler_params=pltpu.CompilerParams(vmem_limit_bytes=8 << 20),
    )(images, texts)


def block_kernel(scale_ref, place_ref, image_ref, text_ref, row_ref, col_ref, col_high, col_low):
    tile = 256
    half_scale = scale_ref[0] * (0.5 * LOG2E)
    x, z = place_ref[0], place_ref[1]
    cut = math.exp(-HIGH / 2)
    lift = math.exp((HIGH - LOW) / 2)
    rows, cols = image_ref.shape[0], text_ref.shape[0]
    for r in range(rows // tile):
        high_sum = low_sum = None
        for c in range(cols // tile):
            dots = lax.dot_general(
                image_ref[r * tile : (r + 1) * tile, :],
                text_ref[c * tile : (c + 1) * tile, :],
                (((1,), (1,)), ((), ())),
                preferred_element_type=jnp.float32,
            )
            root = jnp.exp2(dots * half_scale - (HIGH / 2 * LOG2E))
            high = root * root
            low = jnp.minimum(root, cut) * lift
            low = low * low
            high_part = high[:, :128] + high[:, 128:]
            low_part = low[:, :128] + low[:, 128:]
            high_sum = high_part if high_sum is None else high_sum + high_part
            low_sum = low_part if low_sum is None else low_sum + low_part
            at = slice(c * tile, (c + 1) * tile)
            high_col = jnp.sum(high.reshape(tile // 8, 8, tile), axis=0)
            low_col = jnp.sum(low.reshape(tile // 8, 8, tile), axis=0)
            if r == 0:
                col_high[:, at] = high_col
                col_low[:, at] = low_col
            else:
                col_high[:, at] += high_col
                col_low[:, at] += low_col
        place = (lax.rem(x + r, 4) ^ x) * 4
        for e in range(2):
            part = slice(e * 128, (e + 1) * 128)
            row_ref[pl.ds(place + 2 * e, 1), :] = jnp.sum(high_sum[part].T, axis=0, keepdims=True)
            row_ref[pl.ds(place + 2 * e + 1, 1), :] = jnp.sum(low_sum[part].T, axis=0, keepdims=True)
    half = cols // 2
    for e in range(2):
        at = slice(e * half, (e + 1) * half)
        high_col = jnp.sum(col_high[:, at], axis=0, keepdims=True)
        low_col = jnp.sum(col_low[:, at], axis=0, keepdims=True)
        for d in range(8):
            part = slice(64 * d, 64 * d + 64)
            place = (lax.rem(z + d, 8) ^ z) * 2 + e
            col_ref[pl.ds(place, 1), :] = jnp.concatenate([high_col[:, part], low_col[:, part]], axis=1)


def block_sums(logit_scale, place, images, texts):
    rows, cols, depth = images.shape[0], texts.shape[0], images.shape[1]
    return pl.pallas_call(
        block_kernel,
        out_shape=(
            jax.ShapeDtypeStruct((rows // 64, 128), jnp.float32),
            jax.ShapeDtypeStruct((cols // 64, 128), jnp.float32),
        ),
        in_specs=[SMEM, SMEM, VMEM, VMEM],
        out_specs=(VMEM, VMEM),
        scratch_shapes=[pltpu.VMEM((8, cols), jnp.float32), pltpu.VMEM((8, cols), jnp.float32)],
        compiler_params=pltpu.CompilerParams(vmem_limit_bytes=24 << 20),
        cost_estimate=pl.CostEstimate(
            flops=2 * rows * cols * depth,
            bytes_accessed=2 * (rows + cols) * depth,
            transcendentals=rows * cols,
        ),
    )(logit_scale, place, images, texts)


def fetch(block, axis, size, apart):
    return lax.ppermute(block, axis, [((i + apart) % size, i) for i in range(size)])


def send(block, axis, size, apart):
    return fetch(block, axis, size, -apart)


def gather_images(own):
    flip = lax.ppermute(own, ("yh", "yl"), FLIP_Y)
    half = own.shape[0] // 2
    above = fetch(own, "x", 4, 1)
    below = fetch(own, "x", 4, -1)
    far_above = fetch(jnp.concatenate([flip, above[:half]], 0), "x", 4, 1)
    far_below = fetch(jnp.concatenate([flip, below[half:]], 0), "x", 4, -1)
    rows = 2 * half
    flip_above, flip_below = far_above[:rows], far_below[:rows]
    flip_far_a = fetch(flip_above[:half], "x", 4, 1)
    flip_far_b = fetch(flip_below[half:], "x", 4, -1)
    return jnp.concatenate(
        [own, flip, above, flip_above, far_above[rows:], far_below[rows:], flip_far_a, flip_far_b, below, flip_below],
        0,
    )


def gather_texts(own):
    half = own.shape[0] // 2
    p2, m2 = fetch(own, "z", 8, 2), fetch(own, "z", 8, -2)
    p1, m1 = fetch(own, "z", 8, 1), fetch(own, "z", 8, -1)
    p3, m3 = fetch(p2, "z", 8, 1), fetch(m2, "z", 8, -1)
    p4, m4 = fetch(p2[:half], "z", 8, 2), fetch(m2[half:], "z", 8, -2)
    mine = jnp.concatenate([own, p1, p2, p3, p4, m4, m3, m2, m1], 0)
    other = lax.ppermute(mine, "c", ((0, 1), (1, 0)))
    return jnp.concatenate([mine, other], 0)


def swap(block, axis, size, mask):
    return lax.ppermute(block, axis, [(i, i ^ mask) for i in range(size)])


def reduce_sums(rows, cols):
    for mask in (2, 1):
        half = rows.shape[0] // 2
        row_in = swap(rows[half:], "x", 4, mask)
        other = cols.shape[0] // 2
        col_in = swap(cols[other:], "z", 8, 2 * mask)
        rows, cols = lax.optimization_barrier((rows[:half] + row_in, cols[:other] + col_in))
    row_in = lax.ppermute(rows[2:], ("yh", "yl"), FLIP_Y)
    col_in = swap(cols[2:], "z", 8, 1)
    rows, cols = lax.optimization_barrier((rows[:2] + row_in, cols[:2] + col_in))
    yl = lax.axis_index("yl")
    low, high = rows[:, :64], rows[:, 64:]
    row_in = swap(jnp.where(yl == 0, high, low), "yl", 2, 1)
    col_in = swap(cols[1:], "c", 2, 1)
    rows = jnp.where(yl == 0, low, high) + row_in
    cols = cols[:1] + col_in
    return rows, jnp.concatenate([cols[:, :64], cols[:, 64:]], axis=0)


def log_sum(sums):
    high, low = sums[0], sums[1]
    return jnp.where(high > math.exp(-HIGH), jnp.log(high) + HIGH, jnp.log(low) + LOW)


def on_device(images, texts, logit_scale):
    image_unit, text_unit = normalise(images, texts)
    rows = text_unit.shape[0]
    all_images = gather_images(image_unit)
    all_texts = gather_texts(text_unit)
    place = jnp.stack([lax.axis_index("x"), lax.axis_index("z")]).astype(jnp.int32)
    row_sums, col_sums = block_sums(logit_scale, place, all_images, all_texts)
    image_own = lax.dynamic_slice_in_dim(image_unit, lax.axis_index("yl") * rows, rows, 0)
    diagonal = (
        jnp.sum(image_own.astype(jnp.float32) * text_unit.astype(jnp.float32), axis=1) * logit_scale[0]
    )
    row_sums, col_sums = reduce_sums(row_sums, col_sums)
    image_lse, text_lse = log_sum(row_sums), log_sum(col_sums)
    return (image_lse - diagonal, text_lse - diagonal)


def solution(mesh):
    fine = Mesh(mesh.devices.reshape(4, 8, 2, 2, 2), ("x", "z", "yh", "c", "yl"))
    dp = ("x", "z", "yh", "c")
    in_specs = (P(dp, None), P(dp + ("yl",), None), P())
    out_specs = (P(dp + ("yl",)), P(dp + ("yl",)))
    return jax.shard_map(
        on_device, mesh=fine, in_specs=in_specs, out_specs=out_specs, check_vma=False
    )
```

```python
import functools
import math

import jax
import jax.numpy as jnp
from jax import lax
from jax.experimental import pallas as pl
from jax.experimental.pallas import tpu as pltpu
from jax.sharding import Mesh
from jax.sharding import PartitionSpec as P


HIGH = 40.0
LOW = -60.0
LOG2E = math.log2(math.e)
VMEM = pl.BlockSpec(memory_space=pltpu.VMEM)
SMEM = pl.BlockSpec(memory_space=pltpu.SMEM)
IMAGES = ("image", "flip", "near", "second", "flip_far", "near_back", "flip_back")
IMAGE_ORDER = (
    (0, 0, 128),
    (1, 0, 128),
    (2, 0, 128),
    (3, 0, 128),
    (3, 256, 384),
    (4, 0, 128),
    (5, 0, 128),
    (6, 0, 128),
)
FLIP_Y = ((0, 3), (3, 0), (1, 2), (2, 1))


def normalise_kernel(images_ref, texts_ref, image_unit_ref, text_unit_ref, both_ref):
    for source, target in ((images_ref, image_unit_ref), (texts_ref, text_unit_ref)):
        wide = source[...].astype(jnp.float32)
        squares = jnp.sum(wide * wide, axis=1, keepdims=True)
        target[...] = (wide * lax.rsqrt(squares + 1.0)).astype(jnp.bfloat16)
    rows = images_ref.shape[0]
    both_ref[:rows, :] = image_unit_ref[...]
    both_ref[rows:, :] = text_unit_ref[...]


def normalise(images, texts):
    return pl.pallas_call(
        normalise_kernel,
        out_shape=(
            jax.ShapeDtypeStruct(images.shape, jnp.bfloat16),
            jax.ShapeDtypeStruct(texts.shape, jnp.bfloat16),
            jax.ShapeDtypeStruct((images.shape[0] + texts.shape[0], images.shape[1]), jnp.bfloat16),
        ),
        in_specs=[VMEM, VMEM],
        out_specs=(VMEM, VMEM, VMEM),
        compiler_params=pltpu.CompilerParams(vmem_limit_bytes=4 << 20),
    )(images, texts)


def copy_kernel(plan, *refs):
    sources, targets = refs[: -len(plan)], refs[-len(plan) :]
    for pieces, target in zip(plan, targets, strict=True):
        at = 0
        for source, start, stop in pieces:
            target[at : at + stop - start, :] = sources[source][start:stop, :]
            at += stop - start


def rearrange(sources, plan):
    width = sources[0].shape[1]
    return pl.pallas_call(
        functools.partial(copy_kernel, plan),
        out_shape=tuple(
            jax.ShapeDtypeStruct((sum(stop - start for _, start, stop in pieces), width), jnp.bfloat16)
            for pieces in plan
        ),
        in_specs=[VMEM] * len(sources),
        out_specs=(VMEM,) * len(plan),
        compiler_params=pltpu.CompilerParams(vmem_limit_bytes=2 << 20),
    )(*sources)


def block_kernel(scale_ref, *refs):
    image_refs, text_refs = refs[: len(IMAGES)], refs[len(IMAGES) : -6]
    row_ref, col_ref, image_ref, text_ref, col_high, col_low = refs[-6:]
    text_pieces = [(ref, (0, ref.shape[0])) for ref in text_refs]
    image_pieces = [(image_refs[i], (start, stop)) for i, start, stop in IMAGE_ORDER]
    tile = 256
    half_scale = scale_ref[0] * (0.5 * LOG2E)
    x, z = lax.axis_index("x"), lax.axis_index("z")
    side = 2 * lax.axis_index("c") - 1
    cut = math.exp(-HIGH / 2)
    lift = math.exp((HIGH - LOW) / 2)
    for pieces, whole in ((text_pieces, text_ref), (image_pieces, image_ref)):
        at = 0
        for piece, (start, stop) in pieces:
            whole[at : at + stop - start, :] = piece[start:stop, :]
            at += stop - start
    rows, cols = image_ref.shape[0], text_ref.shape[0]
    for r in range(rows // tile):
        high_sum = low_sum = None
        for c in range(cols // tile):
            dots = lax.dot_general(
                image_ref[r * tile : (r + 1) * tile, :],
                text_ref[c * tile : (c + 1) * tile, :],
                (((1,), (1,)), ((), ())),
                preferred_element_type=jnp.float32,
            )
            root = jnp.exp2(dots * half_scale - (HIGH / 2 * LOG2E))
            high = root * root
            low = jnp.minimum(root, cut) * lift
            low = low * low
            high_part = high[:, :128] + high[:, 128:]
            low_part = low[:, :128] + low[:, 128:]
            high_sum = high_part if high_sum is None else high_sum + high_part
            low_sum = low_part if low_sum is None else low_sum + low_part
            at = slice(c * tile, (c + 1) * tile)
            high_col = jnp.sum(high.reshape(tile // 8, 8, tile), axis=0)
            low_col = jnp.sum(low.reshape(tile // 8, 8, tile), axis=0)
            if r == 0:
                col_high[:, at] = high_col
                col_low[:, at] = low_col
            else:
                col_high[:, at] += high_col
                col_low[:, at] += low_col
        apart = (0, side, 2, -side)[r]
        place = (lax.rem(x + 4 + apart, 4) ^ x) * 4
        for e in range(2):
            part = slice(e * 128, (e + 1) * 128)
            row_ref[pl.ds(place + 2 * e, 1), :] = jnp.sum(high_sum[part].T, axis=0, keepdims=True)
            row_ref[pl.ds(place + 2 * e + 1, 1), :] = jnp.sum(low_sum[part].T, axis=0, keepdims=True)
    high_col = jnp.sum(col_high[...], axis=0, keepdims=True)
    low_col = jnp.sum(col_low[...], axis=0, keepdims=True)
    for i, (apart, e) in enumerate(
        [(0, 0), (0, 1)]
        + [(k * side, e) for k in (1, 2, 3) for e in (0, 1)]
        + [(4, 0)]
        + [(-k * side, e) for k in (1, 2, 3) for e in (1, 0)]
        + [(4, 1)]
    ):
        part = slice(64 * i, 64 * i + 64)
        place = (lax.rem(z + 8 + apart, 8) ^ z) * 2 + e
        col_ref[pl.ds(place, 1), :] = jnp.concatenate([high_col[:, part], low_col[:, part]], axis=1)


def block_sums(logit_scale, images, texts):
    rows = sum(stop - start for _, start, stop in IMAGE_ORDER)
    cols, depth = sum(t.shape[0] for t in texts), texts[0].shape[1]
    return pl.pallas_call(
        block_kernel,
        out_shape=(
            jax.ShapeDtypeStruct((rows // 64, 128), jnp.float32),
            jax.ShapeDtypeStruct((cols // 64, 128), jnp.float32),
        ),
        in_specs=[SMEM] + [VMEM] * (len(images) + len(texts)),
        out_specs=(VMEM, VMEM),
        scratch_shapes=[
            pltpu.VMEM((rows, depth), jnp.bfloat16),
            pltpu.VMEM((cols, depth), jnp.bfloat16),
            pltpu.VMEM((8, cols), jnp.float32),
            pltpu.VMEM((8, cols), jnp.float32),
        ],
        compiler_params=pltpu.CompilerParams(vmem_limit_bytes=10 << 20),
        cost_estimate=pl.CostEstimate(
            flops=2 * rows * cols * depth,
            bytes_accessed=2 * (rows + cols) * depth,
            transcendentals=rows * cols,
        ),
    )(logit_scale, *images, *texts)


def across(block):
    return lax.ppermute(block, "c", ((0, 1), (1, 0)))


def step(block, axis, size, apart):
    route = []
    for i in range(size):
        route += [(2 * i, 2 * ((i + apart) % size)), (2 * i + 1, 2 * ((i - apart) % size) + 1)]
    return lax.ppermute(block, (axis, "c"), route)


def gather(image, text, both):
    rows, cols = image.shape[0], text.shape[0]
    other = across(both)
    with jax.named_scope("flip"):
        flip = lax.ppermute(image, ("yh", "yl"), FLIP_Y)
    chip_image, chip_text = rearrange(
        (both, other),
        (((0, 0, rows), (1, 0, rows)), ((0, rows, rows + cols), (1, rows, rows + cols))),
    )
    with jax.named_scope("x_one"):
        near = step(chip_image, "x", 4, 1)
    with jax.named_scope("z_two"):
        two = step(chip_text, "z", 8, 2)
    with jax.named_scope("z_one"):
        one = step(chip_text, "z", 8, 1)
    flip_other = across(flip)
    onward, near_away = rearrange(
        (flip, flip_other, near),
        (((0, 0, rows), (1, 0, rows), (2, 0, rows)), ((2, rows, 2 * rows),)),
    )
    with jax.named_scope("x_two"):
        second = step(onward, "x", 4, 1)
    near_back = across(near_away)
    (two_half,) = rearrange((two,), (((0, 0, cols),),))
    with jax.named_scope("z_four"):
        four = step(two_half, "z", 8, 2)
    with jax.named_scope("z_three"):
        three = step(two, "z", 8, 1)
    one_back, two_back = across(one), across(two)
    flip_near, flip_away = rearrange((second,), (((0, 0, rows),), ((0, rows, 2 * rows),)))
    with jax.named_scope("x_three"):
        flip_far = step(flip_near, "x", 4, 1)
    flip_back = across(flip_away)
    three_back, four_back = across(three), across(four)
    images = (image, flip, near, second, flip_far, near_back, flip_back)
    texts = (chip_text, one, two, three, four, one_back, two_back, three_back, four_back)
    return images, texts


def swap(block, axis, size, mask):
    return lax.ppermute(block, axis, [(i, i ^ mask) for i in range(size)])


def reduce_sums(rows, cols):
    for mask in (2, 1):
        half = rows.shape[0] // 2
        row_in = swap(rows[half:], "x", 4, mask)
        other = cols.shape[0] // 2
        col_in = swap(cols[other:], "z", 8, 2 * mask)
        rows, cols = lax.optimization_barrier((rows[:half] + row_in, cols[:other] + col_in))
    row_in = lax.ppermute(rows[2:], ("yh", "yl"), FLIP_Y)
    col_in = swap(cols[2:], "z", 8, 1)
    rows, cols = lax.optimization_barrier((rows[:2] + row_in, cols[:2] + col_in))
    yl = lax.axis_index("yl")
    low, high = rows[:, :64], rows[:, 64:]
    row_in = swap(jnp.where(yl == 0, high, low), "yl", 2, 1)
    col_in = swap(cols[1:], "c", 2, 1)
    rows = jnp.where(yl == 0, low, high) + row_in
    cols = cols[:1] + col_in
    return rows, jnp.concatenate([cols[:, :64], cols[:, 64:]], axis=0)


def log_sum(sums):
    high, low = sums[0], sums[1]
    return jnp.where(high > math.exp(-HIGH), jnp.log(high) + HIGH, jnp.log(low) + LOW)


def on_device(images, texts, logit_scale):
    image_unit, text_unit, both = normalise(images, texts)
    rows = text_unit.shape[0]
    all_images, all_texts = gather(image_unit, text_unit, both)
    row_sums, col_sums = block_sums(logit_scale, all_images, all_texts)
    image_own = lax.dynamic_slice_in_dim(image_unit, lax.axis_index("yl") * rows, rows, 0)
    diagonal = (
        jnp.sum(image_own.astype(jnp.float32) * text_unit.astype(jnp.float32), axis=1) * logit_scale[0]
    )
    row_sums, col_sums = reduce_sums(row_sums, col_sums)
    image_lse, text_lse = log_sum(row_sums), log_sum(col_sums)
    return (image_lse - diagonal, text_lse - diagonal)


def solution(mesh):
    fine = Mesh(mesh.devices.reshape(4, 8, 2, 2, 2), ("x", "z", "yh", "c", "yl"))
    dp = ("x", "z", "yh", "c")
    in_specs = (P(dp, None), P(dp + ("yl",), None), P())
    out_specs = (P(dp + ("yl",)), P(dp + ("yl",)))
    return jax.shard_map(
        on_device, mesh=fine, in_specs=in_specs, out_specs=out_specs, check_vma=False
    )
```

```python
import functools
import itertools
import math

import jax
import jax.numpy as jnp
from jax import lax
from jax.experimental import pallas as pl
from jax.experimental.pallas import tpu as pltpu
from jax.sharding import Mesh
from jax.sharding import PartitionSpec as P


HIGH = 40.0
LOW = -60.0
LOG2E = math.log2(math.e)
VMEM = pl.BlockSpec(memory_space=pltpu.VMEM)
SMEM = pl.BlockSpec(memory_space=pltpu.SMEM)
IMAGE_ROWS = 128
FLIP_Y = ((0, 3), (3, 0), (1, 2), (2, 1))


def normalise_kernel(images_ref, texts_ref, image_unit_ref, text_unit_ref, both_ref):
    for source, target in ((images_ref, image_unit_ref), (texts_ref, text_unit_ref)):
        wide = source[...].astype(jnp.float32)
        squares = jnp.sum(wide * wide, axis=1, keepdims=True)
        target[...] = (wide * lax.rsqrt(squares + 1.0)).astype(jnp.bfloat16)
    rows = images_ref.shape[0]
    both_ref[:rows, :] = image_unit_ref[...]
    both_ref[rows:, :] = text_unit_ref[...]


def normalise(images, texts):
    return pl.pallas_call(
        normalise_kernel,
        out_shape=(
            jax.ShapeDtypeStruct(images.shape, jnp.bfloat16),
            jax.ShapeDtypeStruct(texts.shape, jnp.bfloat16),
            jax.ShapeDtypeStruct((images.shape[0] + texts.shape[0], images.shape[1]), jnp.bfloat16),
        ),
        in_specs=[VMEM, VMEM],
        out_specs=(VMEM, VMEM, VMEM),
        compiler_params=pltpu.CompilerParams(vmem_limit_bytes=4 << 20),
    )(images, texts)


def copy_kernel(plan, *refs):
    sources, targets = refs[: -len(plan)], refs[-len(plan) :]
    for pieces, target in zip(plan, targets, strict=True):
        at = 0
        for source, start, stop in pieces:
            target[at : at + stop - start, :] = sources[source][start:stop, :]
            at += stop - start


def rearrange(sources, plan):
    width = sources[0].shape[1]
    return pl.pallas_call(
        functools.partial(copy_kernel, plan),
        out_shape=tuple(
            jax.ShapeDtypeStruct((sum(stop - start for _, start, stop in pieces), width), jnp.bfloat16)
            for pieces in plan
        ),
        in_specs=[VMEM] * len(sources),
        out_specs=(VMEM,) * len(plan),
        compiler_params=pltpu.CompilerParams(vmem_limit_bytes=2 << 20),
    )(*sources)


def block_kernel(scale_ref, *refs):
    keep_ref, away_ref, row_ref, col_ref, image_ref, text_ref, col_high, col_low = refs[-8:]
    image_pieces = [(ref, IMAGE_ROWS) for ref in refs[:8]]
    text_pieces = [(ref, ref.shape[0]) for ref in refs[8:-8]]
    tile = 256
    half_scale = scale_ref[0] * (0.5 * LOG2E)
    x, z, core = lax.axis_index("x"), lax.axis_index("z"), lax.axis_index("c")
    side = 2 * core - 1
    cut = math.exp(-HIGH / 2)
    lift = math.exp((HIGH - LOW) / 2)
    for pieces, whole in ((text_pieces, text_ref), (image_pieces, image_ref)):
        at = 0
        for piece, count in pieces:
            whole[at : at + count, :] = piece[:count, :]
            at += count
    rows, cols = image_ref.shape[0], text_ref.shape[0]
    for r in range(rows // tile):
        high_sum = low_sum = None
        for c in range(cols // tile):
            dots = lax.dot_general(
                image_ref[r * tile : (r + 1) * tile, :],
                text_ref[c * tile : (c + 1) * tile, :],
                (((1,), (1,)), ((), ())),
                preferred_element_type=jnp.float32,
            )
            root = jnp.exp2(dots * half_scale - (HIGH / 2 * LOG2E))
            high = root * root
            low = jnp.minimum(root, cut) * lift
            low = low * low
            high_part = high[:, :128] + high[:, 128:]
            low_part = low[:, :128] + low[:, 128:]
            high_sum = high_part if high_sum is None else high_sum + high_part
            low_sum = low_part if low_sum is None else low_sum + low_part
            at = slice(c * tile, (c + 1) * tile)
            high_col = jnp.sum(high.reshape(tile // 8, 8, tile), axis=0)
            low_col = jnp.sum(low.reshape(tile // 8, 8, tile), axis=0)
            if r == 0:
                col_high[:, at] = high_col
                col_low[:, at] = low_col
            else:
                col_high[:, at] += high_col
                col_low[:, at] += low_col
        apart = (0, side, 2, -side)[r]
        place = (lax.rem(x + 4 + apart, 4) ^ x) * 4
        for e in range(2):
            part = slice(e * 128, (e + 1) * 128)
            row_ref[pl.ds(place + 2 * e, 1), :] = jnp.sum(high_sum[part].T, axis=0, keepdims=True)
            row_ref[pl.ds(place + 2 * e + 1, 1), :] = jnp.sum(low_sum[part].T, axis=0, keepdims=True)
    high_col = jnp.sum(col_high[...], axis=0, keepdims=True)
    low_col = jnp.sum(col_low[...], axis=0, keepdims=True)
    for i, (apart, e) in enumerate(
        [(0, 0), (0, 1)]
        + [(k * side, e) for k in (1, 2, 3) for e in (0, 1)]
        + [(4, 0)]
        + [(-k * side, e) for k in (1, 2, 3) for e in (1, 0)]
        + [(4, 1)]
    ):
        part = slice(64 * i, 64 * i + 64)
        place = (lax.rem(z + 8 + apart, 8) ^ z) * 2 + (core ^ e)
        col_ref[pl.ds(place, 1), :] = jnp.concatenate([high_col[:, part], low_col[:, part]], axis=1)

    @pl.when(core == 0)
    def _():
        keep_ref[...], away_ref[...] = row_ref[...], col_ref[...]

    @pl.when(core == 1)
    def _():
        keep_ref[...], away_ref[...] = col_ref[...], row_ref[...]


def block_sums(logit_scale, images, texts):
    rows = IMAGE_ROWS * len(images)
    cols, depth = sum(t.shape[0] for t in texts), texts[0].shape[1]
    return pl.pallas_call(
        block_kernel,
        out_shape=(
            jax.ShapeDtypeStruct((rows // 64, 128), jnp.float32),
            jax.ShapeDtypeStruct((cols // 64, 128), jnp.float32),
        ),
        in_specs=[SMEM] + [VMEM] * (len(images) + len(texts)),
        out_specs=(VMEM, VMEM),
        scratch_shapes=[
            pltpu.VMEM((rows // 64, 128), jnp.float32),
            pltpu.VMEM((cols // 64, 128), jnp.float32),
            pltpu.VMEM((rows, depth), jnp.bfloat16),
            pltpu.VMEM((cols, depth), jnp.bfloat16),
            pltpu.VMEM((8, cols), jnp.float32),
            pltpu.VMEM((8, cols), jnp.float32),
        ],
        compiler_params=pltpu.CompilerParams(vmem_limit_bytes=10 << 20),
        cost_estimate=pl.CostEstimate(
            flops=2 * rows * cols * depth,
            bytes_accessed=2 * (rows + cols) * depth,
            transcendentals=rows * cols,
        ),
    )(logit_scale, *images, *texts)


def across(block):
    return lax.ppermute(block, "c", ((0, 1), (1, 0)))


def step(block, axis, size, apart):
    route = []
    for i in range(size):
        route += [(2 * i, 2 * ((i + apart) % size)), (2 * i + 1, 2 * ((i - apart) % size) + 1)]
    return lax.ppermute(block, (axis, "c"), route)


def gather(image, text, both):
    rows, cols = image.shape[0], text.shape[0]
    other = across(both)
    flip = lax.ppermute(image, ("yh", "yl"), FLIP_Y)
    chip_image, chip_text = rearrange(
        (both, other),
        (((0, 0, rows), (1, 0, rows)), ((0, rows, rows + cols), (1, rows, rows + cols))),
    )
    near = step(chip_image, "x", 4, 1)
    two = step(chip_text, "z", 8, 2)
    one = step(chip_text, "z", 8, 1)
    flip_other = across(flip)
    near_here, near_away = rearrange((near,), (((0, 0, rows),), ((0, rows, 2 * rows),)))
    far = step(near_here, "x", 4, 1)
    (chip_flip,) = rearrange((flip, flip_other), (((0, 0, rows), (1, 0, rows)),))
    flip_near = step(chip_flip, "x", 4, 1)
    near_back = across(near_away)
    flip_far = lax.ppermute(far, ("yh", "yl"), FLIP_Y)
    (two_half,) = rearrange((two,), (((0, 0, cols),),))
    four = step(two_half, "z", 8, 2)
    three = step(two, "z", 8, 1)
    one_back, two_back = across(one), across(two)
    (flip_away,) = rearrange((flip_near,), (((0, rows, 2 * rows),),))
    flip_back = across(flip_away)
    three_back, four_back = across(three), across(four)
    images = (image, flip, near_here, flip_near, far, flip_far, near_back, flip_back)
    texts = (chip_text, one, two, three, four, one_back, two_back, three_back, four_back)
    return images, texts


def each_core(block, row_step, col_step):
    route = []
    for x, z, y in itertools.product(range(4), range(8), range(4)):
        for core, move in enumerate((row_step, col_step)):
            if move is not None:
                source, target = (
                    ((i * 8 + j) * 2 + k // 2) * 4 + core * 2 + k % 2 for i, j, k in ((x, z, y), move(x, z, y))
                )
                route.append((source, target))
    return lax.ppermute(block, ("x", "z", "yh", "c", "yl"), route)


def reduce_sums(keep, away):
    core, yl = lax.axis_index("c"), lax.axis_index("yl")
    other = across(away)
    sums = jnp.concatenate([keep + jnp.where(core == 0, 0.0, other), other], axis=1)
    for row_step, col_step in (
        (lambda x, z, y: (x ^ 2, z, y), lambda x, z, y: (x, z ^ 4, y)),
        (lambda x, z, y: (x ^ 1, z, y), lambda x, z, y: (x, z ^ 2, y)),
        (lambda x, z, y: (x, z, y ^ 3), lambda x, z, y: (x, z ^ 1, y)),
    ):
        half = sums.shape[0] // 2
        sums = sums[:half] + each_core(sums[half:], row_step, col_step)
    low = jnp.concatenate([sums[:, :64], sums[:, 128:192]], axis=1)
    high = jnp.concatenate([sums[:, 64:128], sums[:, 192:]], axis=1)
    rows = each_core(jnp.where(yl == 0, high, low), lambda x, z, y: (x, z, y ^ 1), None)
    rows = rows + jnp.where(yl == 0, low, high)
    cols = [jnp.concatenate([sums[i : i + 1, :64], sums[i : i + 1, 64:128]], axis=0) for i in range(2)]
    other = across(jnp.where(core == 0, rows[:, 64:], cols[0]))
    return jnp.where(core == 0, rows[:, :64], other), jnp.where(core == 0, other, cols[1])


def log_sum(sums):
    high, low = sums[0], sums[1]
    return jnp.where(high > math.exp(-HIGH), jnp.log(high) + HIGH, jnp.log(low) + LOW)


def on_device(images, texts, logit_scale):
    image_unit, text_unit, both = normalise(images, texts)
    rows = text_unit.shape[0]
    all_images, all_texts = gather(image_unit, text_unit, both)
    row_sums, col_sums = block_sums(logit_scale, all_images, all_texts)
    image_own = lax.dynamic_slice_in_dim(image_unit, lax.axis_index("yl") * rows, rows, 0)
    diagonal = (
        jnp.sum(image_own.astype(jnp.float32) * text_unit.astype(jnp.float32), axis=1) * logit_scale[0]
    )
    row_sums, col_sums = reduce_sums(row_sums, col_sums)
    image_lse, text_lse = log_sum(row_sums), log_sum(col_sums)
    return (image_lse - diagonal, text_lse - diagonal)


def solution(mesh):
    fine = Mesh(mesh.devices.reshape(4, 8, 2, 2, 2), ("x", "z", "yh", "c", "yl"))
    dp = ("x", "z", "yh", "c")
    in_specs = (P(dp, None), P(dp + ("yl",), None), P())
    out_specs = (P(dp + ("yl",)), P(dp + ("yl",)))
    return jax.shard_map(
        on_device, mesh=fine, in_specs=in_specs, out_specs=out_specs, check_vma=False
    )
```
